32 devices in a mesh: dp: 8 (over y, x, core), tensor: 4 (over z).
Axes of the slice: x: 2, y: 2, z: 4, core: 2. Of those that a mesh axis runs over, the one named last changes fastest.
Arguments:
- tokens: bfloat16 [256, 6144], P('dp', 'tensor'), may hold values from -6 to 6
- router_weight: bfloat16 [6144, 8], P('tensor'), may hold values from -0.078125 to 0.078125
- expert_ids: int32 [256, 2], P('dp'), may hold values from 0 to 7, all different within a row; in each aligned block of 32 rows (0 to 31, 32 to 63, ...) at most 12 rows name the same one
- w_gate: bfloat16 [8, 6144, 12288], P('dp', None, 'tensor'), may hold values from -0.078125 to 0.078125
- w_up: bfloat16 [8, 6144, 12288], P('dp', None, 'tensor'), may hold values from -0.078125 to 0.078125
- w_down: bfloat16 [8, 12288, 6144], P('dp', 'tensor'), may hold values from -0.0546875 to 0.0546875
Outputs:
- moe_out: bfloat16 [256, 6144], P('dp', 'tensor')
The draws below stay inside these ranges and needn't reach their ends.
Inputs may be any that keep to these rules, and one draw needn't show every extreme that they name: `expert_ids`: the two experts of a token differ. In each aligned block of 32 rows (the rows of one index of dp) no expert is named by more than 12 rows, a bound that some blocks reach.
All inputs are finite; a program needn't handle non-finite values.
Results may differ from the reference program's by a relative error of at most 0.022.
Values may be sent and summed in bfloat16 or wider, within the bound.
A program may use at most 192 MiB of HBM per device.

```python
import math
import jax
import jax.numpy as jnp
import numpy as np
from jax import lax

D = 6144
FF = 12288
EXPERTS = 8
TOK_DP = 32
CAP = 12
TOKENS = 256
N_DP = 8
N_TENSOR = 4


def block_scale(stream_key, dims, cuts, low, high):
    level, own = 1.0, jax.random.fold_in(stream_key, 6)
    for dim, blocks in cuts:
        draws = jnp.exp(jax.random.uniform(jax.random.fold_in(own, dim), (blocks,), jnp.float32, low / len(cuts), high / len(cuts)))
        level = level * jnp.repeat(draws, dims[dim] // blocks).reshape([-1 if axis == dim else 1 for axis in range(len(dims))])
    return level


def assign_block(rng, own, number, rows, amount, top, bound, slope):
    ranking = jax.random.permutation(rng, amount)
    packed, ordinary = portions_of(amount, rows * top, bound, slope, True), portions_of(amount, rows * top, bound, slope, False)
    places = jnp.arange(amount)

    def named(lengths, offset_by):
        used = int((lengths > 0).sum())
        fixed = max(1, used // 4)
        moved = fixed + (places - fixed + offset_by * (used - fixed)) % max(1, amount - fixed)
        return jnp.zeros((amount,), jnp.int32).at[ranking[jnp.where(places < fixed, places, moved)]].set(jnp.asarray(lengths, jnp.int32))

    lengths = jnp.where(number % 4 == 0, named(packed, number // 4), named(ordinary, number - number // 4 - 1))
    mixed = jax.random.permutation(jax.random.fold_in(own, 3), amount)
    donor, taker = mixed[0:amount // 2 * 2:2], mixed[1:amount // 2 * 2:2]
    slack = jnp.minimum(lengths[donor] - 1, bound - lengths[taker]) // 2
    slack = jnp.where((donor == ranking[0]) | (taker == ranking[0]) | (lengths[taker] == 0), 0, jnp.maximum(slack, 0))
    moved = jax.random.randint(jax.random.fold_in(own, 4), (amount // 2,), 0, 1 << 20) % (slack + 1)
    lengths = lengths.at[donor].add(-moved).at[taker].add(moved)
    labels = jnp.searchsorted(jnp.cumsum(lengths), jnp.arange(rows * top), side="right").astype(jnp.int32)
    grid = labels.reshape(top, rows).T
    grid = grid[jax.random.permutation(jax.random.fold_in(own, 1), rows)]
    offset_by = jax.random.randint(jax.random.fold_in(own, 2), (rows, 1), 0, top)
    return jnp.take_along_axis(grid, (jnp.arange(top)[None, :] + offset_by) % top, axis=1)


def portions_of(number_of, total, most, lean, full):
    portions = [(1 << 20) // math.isqrt(standing ** lean) + 1 for standing in range(1, number_of + 1)]
    largest = most if full else min(most, max(-(-total // number_of), total * portions[0] // sum(portions)))
    least = 1 if total - largest >= number_of - 1 else 0
    given, rest = [largest] + [least] * (number_of - 1), total - largest - least * (number_of - 1)
    while rest > 0:
        candidates = [i for i in range(1, number_of) if given[i] < largest] or [i for i in range(1, number_of) if given[i] < most]
        whole, budget = sum([portions[i] for i in candidates]), rest
        for i in candidates:
            addition = min(most - given[i], max(1, budget * portions[i] // whole), rest)
            given[i] = given[i] + addition
            rest = rest - addition
    return np.array(given)


def gaussian(rng, dims, deviation, reach, split=(), kind=jnp.bfloat16):
    values = deviation * jax.random.normal(rng, dims, jnp.float32)
    if split:
        values = values * block_scale(rng, dims, split, -0.22, 0.18)
    return jnp.clip(values, -reach, reach).astype(kind)


def setup_inputs(seed: int = 0) -> dict:
    key_of = jax.random.split(jax.random.key(seed), 7)
    tokens = gaussian(key_of[0], (TOKENS, D), 1.0, 6.0, ((0, 8), (1, 4)))
    router_weight = gaussian(key_of[1], (D, EXPERTS), D ** -0.5, 0.078125, ((0, 4),))
    expert_ids_keys = jax.random.split(jax.random.fold_in(key_of[2], 1), TOKENS // TOK_DP)
    expert_ids_turns = jax.random.permutation(jax.random.fold_in(key_of[2], 3), TOKENS // TOK_DP)
    expert_ids = jax.vmap(lambda own, number: assign_block(jax.random.fold_in(key_of[2], 2), own, number, TOK_DP, EXPERTS, 2, CAP, 2))(expert_ids_keys, expert_ids_turns).reshape((TOKENS, 2))
    w_gate = gaussian(key_of[3], (N_DP, D, FF // (N_DP // EXPERTS)), D ** -0.5, 0.078125, ((0, 8), (2, 4)))
    w_up = gaussian(key_of[4], (N_DP, D, FF // (N_DP // EXPERTS)), D ** -0.5, 0.078125, ((0, 8), (2, 4)))
    w_down = gaussian(key_of[5], (N_DP, FF // (N_DP // EXPERTS), D), FF ** -0.5, 0.0546875, ((0, 8), (1, 4)))
    return dict(tokens=tokens, router_weight=router_weight, expert_ids=expert_ids, w_gate=w_gate, w_up=w_up, w_down=w_down)


def expert_block(rows, gate_w, up_w, down_w):
    count = rows.shape[0]
    piece = gate_w.shape[2] // N_TENSOR

    def replica(total, parts):
        g_w, u_w, d_w = parts
        gate = jnp.dot(rows, g_w, preferred_element_type=jnp.float32)
        up = jnp.dot(rows, u_w, preferred_element_type=jnp.float32)
        hidden = (jax.nn.silu(gate) * up).astype(jnp.bfloat16)
        hidden_blocks = hidden.reshape(count, N_TENSOR, piece).transpose(1, 0, 2)
        down_blocks = d_w.reshape(N_TENSOR, piece, D)

        def add_block(acc, pair):
            h_part, d_part = pair
            rounded = lax.optimization_barrier(jnp.dot(h_part, d_part, preferred_element_type=jnp.float32).astype(jnp.bfloat16))
            return acc + rounded.astype(jnp.float32), None

        summed, _ = lax.scan(add_block, jnp.zeros((count, D), jnp.float32), (hidden_blocks, down_blocks))
        share = lax.optimization_barrier(summed.astype(jnp.bfloat16))
        return total + share.astype(jnp.float32), None

    result, _ = lax.scan(replica, jnp.zeros((count, D), jnp.float32), (gate_w, up_w, down_w))
    return result


def reference(tokens, router_weight, expert_ids, w_gate, w_up, w_down):
    groups = N_DP // EXPERTS
    slots_all = N_DP * CAP
    logits = jnp.dot(tokens, router_weight, preferred_element_type=jnp.float32)
    chosen = jnp.take_along_axis(logits, expert_ids.astype(jnp.int32), axis=1)
    first = jax.nn.sigmoid(chosen[:, 0] - chosen[:, 1])
    gates = jnp.stack([first, 1.0 - first], axis=1)
    flat = expert_ids.astype(jnp.int32).reshape(N_DP, TOK_DP * 2)
    onehot = (flat[:, :, None] == jnp.arange(EXPERTS, dtype=jnp.int32)[None, None, :]).astype(jnp.int32)
    ranks = jnp.sum((jnp.cumsum(onehot, axis=1).astype(jnp.int32) - onehot) * onehot, axis=2).astype(jnp.int32)
    blocks = jnp.arange(N_DP, dtype=jnp.int32)[:, None]
    position = (flat * slots_all + blocks * CAP + ranks).astype(jnp.int32).reshape(TOKENS, 2)
    buffers = jnp.zeros((EXPERTS * slots_all, D), jnp.bfloat16)
    buffers = buffers.at[position[:, 0]].set(tokens).at[position[:, 1]].set(tokens)
    buffers = buffers.reshape(EXPERTS, slots_all, D)
    gate_all = w_gate.reshape(EXPERTS, groups, D, -1)
    up_all = w_up.reshape(EXPERTS, groups, D, -1)
    down_all = w_down.reshape(EXPERTS, groups, -1, D)
    outputs = lax.map(lambda parts: expert_block(parts[0], parts[1], parts[2], parts[3]), (buffers, gate_all, up_all, down_all))
    outputs = outputs.reshape(EXPERTS * slots_all, D)
    mixed = gates[:, 0:1] * outputs[position[:, 0]] + gates[:, 1:2] * outputs[position[:, 1]]
    return mixed.astype(jnp.bfloat16)
```

```python
import functools

import jax
import jax.numpy as jnp
from jax import lax
from jax.experimental import pallas as pl
from jax.experimental.pallas import tpu as pltpu
from jax.sharding import PartitionSpec as P

EXPERTS = 8
CAP = 12
PAD = 16
LAG = 4
SLOTS = 16
F32 = jnp.float32
BF16 = jnp.bfloat16


def body(dp, nt, n, sub, pps, slots, tok_ref, rw_ref, ids_ref, wg_ref, wu_ref, wd_ref, out_ref,
         wbuf, rows, packed, hidden, ret_out, ret_in, ztok, zout, zin, own, lg_out, lg_in, hits, wmat,
         w_sem, zt_send, zt_recv, lg_send, lg_recv, d_send, d_recv, r_send, r_recv, zo_send, zo_recv):
    me = lax.axis_index("dp")
    t = lax.axis_index("tensor")
    toks, share = tok_ref.shape
    depth, ff = wg_ref.shape
    width = dp * PAD
    groups = dp // EXPERTS
    chunks = ff // n
    cb = pps * n
    steps = nt * sub
    units = 2 * chunks + steps
    mesh = pl.DeviceIdType.MESH

    def column(s):
        zi = s // sub
        half = nt // 2
        off = jnp.where(zi % 2 == 0, half - zi // 2, half + (zi + 1) // 2)
        q = lax.rem(t + off, nt)
        return q, s % sub

    def load(u, act):
        slot = lax.rem(u, slots)

        @pl.when(u < 2 * chunks)
        def _():
            cols = pl.ds(pl.multiple_of((u // 2) * n, n), n)

            @pl.when(u % 2 == 0)
            def _():
                act(pltpu.make_async_copy(wg_ref.at[:, cols], wbuf.at[slot], w_sem.at[slot]))

            @pl.when(u % 2 == 1)
            def _():
                act(pltpu.make_async_copy(wu_ref.at[:, cols], wbuf.at[slot], w_sem.at[slot]))

        @pl.when((u >= 2 * chunks) & (u < units))
        def _():
            q, j = column(u - 2 * chunks)
            for k in range(pps):
                cols = pl.ds(pl.multiple_of(q * share + j * cb + k * n, n), n)
                act(pltpu.make_async_copy(
                    wd_ref.at[:, cols], wbuf.at[slot, pl.ds(k * ff, ff)], w_sem2(slot, k)))

    def w_sem2(slot, k):
        return w_sem.at[k * slots + slot]

    @pl.loop(0, min(slots, units))
    def _(u):
        load(u, lambda c: c.start())

    rows[...] = jnp.zeros_like(rows)
    ret_in[...] = jnp.zeros_like(ret_in)
    barrier = pltpu.get_barrier_semaphore()

    @pl.loop(1, dp)
    def _(i):
        pl.semaphore_signal(barrier, inc=1, device_id={"dp": lax.rem(me + i, dp)}, device_id_type=mesh)

    @pl.loop(1, nt)
    def _(i):
        pl.semaphore_signal(barrier, inc=1, device_id={"tensor": lax.rem(t + i, nt)}, device_id_type=mesh)

    pl.semaphore_wait(barrier, dp + nt - 2)

    @pl.loop(1, nt)
    def _(i):
        pltpu.make_async_remote_copy(
            tok_ref, ztok.at[t], zt_send.at[i], zt_recv.at[t],
            device_id={"tensor": lax.rem(t + i, nt)}, device_id_type=mesh).start()

    ids = ids_ref[...]
    lane = lax.broadcasted_iota(jnp.int32, (toks, width), 1)
    expert = lane // (PAD * groups)
    rank = (lane % PAD).astype(F32)
    named = [ids[:, k:k + 1] == expert for k in range(2)]
    counts = (named[0] | named[1]).astype(F32).astype(BF16)
    lower = (lax.broadcasted_iota(jnp.int32, (toks, toks), 0)
             > lax.broadcasted_iota(jnp.int32, (toks, toks), 1)).astype(F32).astype(BF16)
    before = jnp.dot(lower, counts, preferred_element_type=F32)
    at_rank = before == rank
    for k in range(2):
        hits[k] = (named[k] & at_rank).astype(F32)
    placing = ((named[0] | named[1]) & at_rank).astype(F32)

    def dispatch(src, value):
        cols = pl.ds(pl.multiple_of(src * share, share), share)
        block = lax.dot_general(placing.astype(BF16), value, (((0,), (0,)), ((), ())),
                                preferred_element_type=F32).astype(BF16)
        packed[src] = block.reshape(dp, PAD, share)
        rows[me, :, cols] = packed[src, me]

        @pl.loop(1, dp)
        def _(i):
            p = lax.rem(me + i, dp)
            pltpu.make_async_remote_copy(
                packed.at[src, p, pl.ds(0, PAD)], rows.at[me, pl.ds(0, PAD), cols],
                d_send.at[src], d_recv.at[src],
                device_id={"dp": p}, device_id_type=mesh).start()

    dispatch(t, tok_ref[...])
    lg_out[...] = jnp.zeros_like(lg_out)
    lg_out[:, 0:EXPERTS] = jnp.dot(tok_ref[...], rw_ref[...], preferred_element_type=F32)
    lg_in[t] = lg_out[...]

    @pl.loop(1, nt)
    def _(i):
        pltpu.make_async_remote_copy(
            lg_out, lg_in.at[t], lg_send.at[i], lg_recv.at[t],
            device_id={"tensor": lax.rem(t + i, nt)}, device_id_type=mesh).start()

    @pl.loop(1, nt)
    def _(i):
        src = lax.rem(t + jnp.where(i % 2 == 1, nt - (i + 1) // 2, i // 2), nt)
        pltpu.make_async_copy(ztok.at[src], ztok.at[src], zt_recv.at[src]).wait()
        dispatch(src, ztok[src])

    @pl.loop(1, nt)
    def _(i):
        src = lax.rem(t + i, nt)
        pltpu.make_async_copy(lg_in.at[src], lg_in.at[src], lg_recv.at[src]).wait()

    logits = jnp.sum(lg_in[...], axis=0)
    lane8 = lax.broadcasted_iota(jnp.int32, logits.shape, 1)
    chosen = [jnp.sum(jnp.where(lane8 == ids[:, k:k + 1], logits, 0.0), axis=1, keepdims=True)
              for k in range(2)]
    first = jax.nn.sigmoid(chosen[0] - chosen[1])
    w = hits[0] * first + hits[1] * (1.0 - first)
    for k in range(3):
        part = w.astype(BF16)
        wmat[k] = part
        w = w - part.astype(F32)

    @pl.loop(0, nt)
    def _(src):
        cols = pl.ds(pl.multiple_of(src * share, share), share)
        view = rows.at[pl.ds(0, dp - 1), pl.ds(0, PAD), cols]
        pltpu.make_async_copy(view, view, d_recv.at[src]).wait()

    @pl.loop(0, chunks)
    def _(c):
        vals = []
        for k in range(2):
            u = 2 * c + k
            slot = lax.rem(u, slots)
            pltpu.make_async_copy(wbuf.at[slot], wbuf.at[slot], w_sem.at[slot]).wait()
            vals.append(jnp.dot(rows[...].reshape(width, depth), wbuf[slot], preferred_element_type=F32))
            load(u + slots, lambda d: d.start())
        gate, up = vals
        hidden[:, pl.ds(pl.multiple_of(c * n, n), n)] = (gate / (1.0 + jnp.exp(-gate)) * up).astype(BF16)

    @pl.loop(0, steps + LAG)
    def _(s):
        @pl.when(s < steps)
        def _():
            u = 2 * chunks + s
            slot = lax.rem(u, slots)
            load(u, lambda d: d.wait())
            for k in range(pps):
                term = jnp.dot(hidden[...], wbuf[slot, pl.ds(k * ff, ff)], preferred_element_type=F32)
                ret_out[s, :, :, pl.ds(k * n, n)] = term.astype(BF16).reshape(dp, PAD, n)
            load(u + slots, lambda d: d.start())
            ret_in[s, me] = ret_out[s, me]

            @pl.loop(1, dp)
            def _(i):
                p = lax.rem(me + i, dp)
                pltpu.make_async_remote_copy(
                    ret_out.at[s, p, pl.ds(0, PAD)], ret_in.at[s, me, pl.ds(0, PAD)],
                    r_send.at[s], r_recv.at[s],
                    device_id={"dp": p}, device_id_type=mesh).start()

        @pl.when(s >= LAG)
        def _():
            b = s - LAG
            q, j = column(b)
            view = ret_in.at[b, pl.ds(0, dp - 1), pl.ds(0, PAD)]
            pltpu.make_async_copy(view, view, r_recv.at[b]).wait()
            back = ret_in[b].reshape(width, cb)
            mixed = jnp.dot(wmat[0], back, preferred_element_type=F32)
            for k in range(1, 3):
                mixed += jnp.dot(wmat[k], back, preferred_element_type=F32)

            @pl.when(b < steps - sub)
            def _():
                zout[b] = mixed.astype(BF16)
                pltpu.make_async_remote_copy(
                    zout.at[b], zin.at[t, j], zo_send.at[b], zo_recv.at[t * sub + j],
                    device_id={"tensor": q}, device_id_type=mesh).start()

            @pl.when(b >= steps - sub)
            def _():
                own[j] = mixed

    @pl.loop(1, nt)
    def _(i):
        src = lax.rem(t + i, nt)

        @pl.loop(0, sub)
        def _(j):
            pltpu.make_async_copy(zin.at[src, j], zin.at[src, j], zo_recv.at[src * sub + j]).wait()
            own[j] += zin[src, j].astype(F32)

    for j in range(sub):
        out_ref[:, j * cb:(j + 1) * cb] = own[j].astype(BF16)

    @pl.loop(1, nt)
    def _(i):
        pltpu.make_async_copy(tok_ref, tok_ref, zt_send.at[i]).wait()
        pltpu.make_async_copy(lg_out, lg_out, lg_send.at[i]).wait()

    @pl.loop(0, nt)
    def _(src):
        view = packed.at[src, pl.ds(0, dp - 1), pl.ds(0, PAD)]
        pltpu.make_async_copy(view, view, d_send.at[src]).wait()

    @pl.loop(0, steps)
    def _(s):
        view = ret_out.at[s, pl.ds(0, dp - 1), pl.ds(0, PAD)]
        pltpu.make_async_copy(view, view, r_send.at[s]).wait()

    @pl.loop(0, steps - sub)
    def _(s):
        pltpu.make_async_copy(zout.at[s], zout.at[s], zo_send.at[s]).wait()


def per_device(dp, nt, tokens, router_weight, expert_ids, w_gate, w_up, w_down):
    toks, share = tokens.shape
    _, depth, ff = w_gate.shape
    n = min(256, ff)
    sub = 1
    while share // (sub * n) * ff > depth or share % (sub * n):
        sub += 1
    pps = share // (sub * n)
    cb = pps * n
    steps = nt * sub
    width = dp * PAD
    slots = SLOTS
    dma = pltpu.SemaphoreType.DMA
    vm = pl.BlockSpec(memory_space=pltpu.VMEM)
    hbm = pl.BlockSpec(memory_space=pltpu.HBM)
    return pl.pallas_call(
        functools.partial(body, dp, nt, n, sub, pps, slots),
        out_shape=jax.ShapeDtypeStruct((toks, share), BF16),
        in_specs=[vm, vm, vm, hbm, hbm, hbm],
        out_specs=vm,
        scratch_shapes=[
            pltpu.VMEM((slots, depth, n), BF16),
            pltpu.VMEM((dp, PAD, depth), BF16),
            pltpu.VMEM((nt, dp, PAD, share), BF16),
            pltpu.VMEM((width, ff), BF16),
            pltpu.VMEM((steps, dp, PAD, cb), BF16),
            pltpu.VMEM((steps, dp, PAD, cb), BF16),
            pltpu.VMEM((nt, toks, share), BF16),
            pltpu.VMEM((steps, toks, cb), BF16),
            pltpu.VMEM((nt, sub, toks, cb), BF16),
            pltpu.VMEM((sub, toks, cb), F32),
            pltpu.VMEM((toks, 128), F32),
            pltpu.VMEM((nt, toks, 128), F32),
            pltpu.VMEM((2, toks, width), F32),
            pltpu.VMEM((3, toks, width), BF16),
            dma((slots * pps,)),
            dma((nt,)), dma((nt,)), dma((nt,)), dma((nt,)),
            dma((nt,)), dma((nt,)), dma((steps,)), dma((steps,)),
            dma((steps,)), dma((steps,)),
        ],
        compiler_params=pltpu.CompilerParams(
            collective_id=0, has_side_effects=True, vmem_limit_bytes=67043328),
    )(tokens, router_weight, expert_ids, w_gate[0], w_up[0], w_down[0])


def solution(mesh):
    return jax.shard_map(
        functools.partial(per_device, mesh.shape["dp"], mesh.shape["tensor"]),
        mesh=mesh,
        in_specs=(
            P("dp", "tensor"),
            P("tensor", None),
            P("dp", None),
            P("dp", None, "tensor"),
            P("dp", None, "tensor"),
            P("dp", "tensor", None),
        ),
        out_specs=P("dp", "tensor"),
        check_vma=False,
    )
```
